16 devices in a mesh: row: 2 (over z), col: 8 (over y, x, core).
Axes of the slice: x: 2, y: 2, z: 2, core: 2. Of those that a mesh axis runs over, the one named last changes fastest.
Arguments:
- w_one: float32 [2, 8, 4, 512, 2048], P('row', 'col')
- w_two: float32 [2, 8, 4, 2048, 512], P('row', 'col')
- inputs: bfloat16 [2, 8, 3, 1024, 512], P('row', 'col')
- targets: bfloat16 [2, 8, 3, 1024, 512], P('row', 'col')
Outputs:
- output 1: float32 [2, 8, 4, 512, 2048], P('row', 'col')
- output 2: float32 [2, 8, 4, 2048, 512], P('row', 'col')
All inputs are finite; a program needn't handle non-finite values.
Results may differ from the reference program's by a relative error of at most 0.00197.
Values are sent between devices in bfloat16 or wider.
A program may use at most 1 GiB of HBM per device.

```python
import jax
import jax.numpy as jnp
from jax import lax

GRID_ROWS = 2
GRID_COLS = 8
LAYERS = 4
NUM_STEPS = 3
BATCH_ROWS = 1024
D_MODEL = 512
D_FF = 2048

LEARN_RATE = 1.5
NORM_EPS = 1e-6
GELU_C = 0.7978845608028654
GELU_K = 0.044715
REPLICA_SPREAD = 0.5


def gelu_value(pre_act):
    tanh_inner = jnp.tanh(GELU_C * (pre_act + GELU_K * pre_act * pre_act * pre_act))
    return 0.5 * pre_act * (1.0 + tanh_inner)


def gelu_slope(pre_act):
    tanh_inner = jnp.tanh(GELU_C * (pre_act + GELU_K * pre_act * pre_act * pre_act))
    return 0.5 * (1.0 + tanh_inner) + 0.5 * pre_act * (1.0 - tanh_inner * tanh_inner) * GELU_C * (1.0 + 3.0 * GELU_K * pre_act * pre_act)


def setup_inputs(seed: int = 0) -> dict:
    root_key = jax.random.key(seed)
    sub_keys = jax.random.split(root_key, 6)
    grid_shape = (GRID_ROWS, GRID_COLS)
    shape_one = (LAYERS, D_MODEL, D_FF)
    shape_two = (LAYERS, D_FF, D_MODEL)
    norm_fac = (1.0 + REPLICA_SPREAD * REPLICA_SPREAD) ** -0.5
    base_one = jax.random.normal(sub_keys[0], shape_one, jnp.float32)
    own_one = jax.random.normal(sub_keys[1], grid_shape + shape_one, jnp.float32)
    w_one = (base_one + REPLICA_SPREAD * own_one) * (norm_fac * D_MODEL ** -0.5)
    base_two = jax.random.normal(sub_keys[2], shape_two, jnp.float32)
    own_two = jax.random.normal(sub_keys[3], grid_shape + shape_two, jnp.float32)
    w_two = (base_two + REPLICA_SPREAD * own_two) * (norm_fac * D_FF ** -0.5)
    data_shape = grid_shape + (NUM_STEPS, BATCH_ROWS, D_MODEL)
    inputs = jax.random.normal(sub_keys[4], data_shape, jnp.float32).astype(jnp.bfloat16)
    targets = jax.random.normal(sub_keys[5], data_shape, jnp.float32).astype(jnp.bfloat16)
    return {'w_one': w_one, 'w_two': w_two, 'inputs': inputs, 'targets': targets}


def local_update(w_one, w_two, x_in, target):
    one_lo = w_one.astype(jnp.bfloat16)
    two_lo = w_two.astype(jnp.bfloat16)
    hidden = x_in
    saved_acts = []
    for layer_idx in range(LAYERS):
        hid_f = hidden.astype(jnp.float32)
        inv_rms = lax.rsqrt(jnp.mean(hid_f * hid_f, axis=-1, keepdims=True) + NORM_EPS)
        normed = hid_f * inv_rms
        normed_lo = normed.astype(jnp.bfloat16)
        pre_act = jnp.dot(normed_lo, one_lo[layer_idx], preferred_element_type=jnp.float32)
        act_lo = gelu_value(pre_act).astype(jnp.bfloat16)
        mlp_out = jnp.dot(act_lo, two_lo[layer_idx], preferred_element_type=jnp.float32)
        saved_acts.append((normed, inv_rms, normed_lo, pre_act, act_lo))
        hidden = (hid_f + mlp_out).astype(jnp.bfloat16)
    d_hidden = (2.0 / (BATCH_ROWS * D_MODEL)) * (hidden.astype(jnp.float32) - target.astype(jnp.float32))
    grads_one = [None] * LAYERS
    grads_two = [None] * LAYERS
    for layer_idx in reversed(range(LAYERS)):
        normed, inv_rms, normed_lo, pre_act, act_lo = saved_acts[layer_idx]
        d_lo = d_hidden.astype(jnp.bfloat16)
        grads_two[layer_idx] = jnp.dot(act_lo.T, d_lo, preferred_element_type=jnp.float32)
        d_act = jnp.dot(d_lo, two_lo[layer_idx].T, preferred_element_type=jnp.float32)
        d_pre = (d_act * gelu_slope(pre_act)).astype(jnp.bfloat16)
        grads_one[layer_idx] = jnp.dot(normed_lo.T, d_pre, preferred_element_type=jnp.float32)
        if layer_idx > 0:
            d_normed = jnp.dot(d_pre, one_lo[layer_idx].T, preferred_element_type=jnp.float32)
            d_hidden = d_hidden + inv_rms * (d_normed - normed * jnp.mean(d_normed * normed, axis=-1, keepdims=True))
    return w_one - LEARN_RATE * jnp.stack(grads_one), w_two - LEARN_RATE * jnp.stack(grads_two)


def gossip_mix(upd_vals):
    wire_vals = upd_vals.astype(jnp.bfloat16)
    mix_sum = upd_vals + jnp.roll(wire_vals, 1, axis=1).astype(jnp.float32)
    mix_sum = mix_sum + jnp.roll(wire_vals, -1, axis=1).astype(jnp.float32)
    mix_sum = mix_sum + jnp.roll(wire_vals, 1, axis=0).astype(jnp.float32)
    mix_sum = mix_sum + jnp.roll(wire_vals, -1, axis=0).astype(jnp.float32)
    return mix_sum / 5.0


def reference(w_one, w_two, inputs, targets):
    n_rep = GRID_ROWS * GRID_COLS
    for step_idx in range(NUM_STEPS):
        flat_one = w_one.reshape((n_rep, LAYERS, D_MODEL, D_FF))
        flat_two = w_two.reshape((n_rep, LAYERS, D_FF, D_MODEL))
        x_step = inputs[:, :, step_idx].reshape((n_rep, BATCH_ROWS, D_MODEL))
        t_step = targets[:, :, step_idx].reshape((n_rep, BATCH_ROWS, D_MODEL))
        upd_one, upd_two = lax.map(lambda packed: local_update(packed[0], packed[1], packed[2], packed[3]), (flat_one, flat_two, x_step, t_step))
        w_one = gossip_mix(upd_one.reshape(w_one.shape))
        w_two = gossip_mix(upd_two.reshape(w_two.shape))
    return w_one, w_two
```

```python
import functools

import jax
import jax.numpy as jnp
from jax import lax
from jax.experimental import pallas as pl
from jax.experimental.pallas import tpu as pltpu
from jax.sharding import PartitionSpec as P

LEARN_RATE = 1.5
NORM_EPS = 1e-6
GELU_C = 0.7978845608028654
GELU_K = 0.044715
TILE = 512
ROWS = 256
F32 = jnp.float32
BF16 = jnp.bfloat16


def gelu_value(z):
    tanh_inner = jnp.tanh(z * (GELU_C + (GELU_C * GELU_K) * (z * z)))
    half = 0.5 * z
    return half + half * tanh_inner


def gelu_slope(z):
    sq = z * z
    tanh_inner = jnp.tanh(z * (GELU_C + (GELU_C * GELU_K) * sq))
    return (0.5 + 0.5 * tanh_inner) + (z * (1.0 - tanh_inner * tanh_inner)) * (0.5 * GELU_C + (1.5 * GELU_C * GELU_K) * sq)


def mm(a, b, dims=((1,), (0,))):
    return lax.dot_general(a, b, (dims, ((), ())), preferred_element_type=F32)


NT = ((1,), (1,))
TN = ((0,), (0,))


def inv_rms_of(x):
    return lax.rsqrt(jnp.mean(x * x, axis=-1, keepdims=True) + NORM_EPS)


def row_blocks(n):
    return [slice(k, k + ROWS) for k in range(0, n, ROWS)]


def params(mib=48):
    return pltpu.CompilerParams(dimension_semantics=('arbitrary',), vmem_limit_bytes=mib << 20)


def cost(flops, nbytes, trans=0):
    return pl.CostEstimate(flops=flops, bytes_accessed=nbytes, transcendentals=trans)


def fwd_body(with_next, h_ref, w1_ref, *rest):
    if with_next:
        w2_ref, z_ref, a_ref, hn_ref, n_scr, acc_scr = rest
    else:
        z_ref, a_ref, n_scr = rest
    j = pl.program_id(0)
    blocks = row_blocks(h_ref.shape[0])

    @pl.when(j == 0)
    def _():
        for r in blocks:
            x = h_ref[r, :].astype(F32)
            n_scr[r, :] = (x * inv_rms_of(x)).astype(BF16)
            if with_next:
                acc_scr[r, :] = jnp.zeros((ROWS, acc_scr.shape[1]), F32)

    w1 = w1_ref[...].astype(BF16)
    if with_next:
        w2 = w2_ref[...].astype(BF16)
    for r in blocks:
        z = mm(n_scr[r, :], w1)
        z_ref[r, :] = z
        a = gelu_value(z).astype(BF16)
        a_ref[r, :] = a
        if with_next:
            acc_scr[r, :] += mm(a, w2)

    if with_next:
        @pl.when(j == pl.num_programs(0) - 1)
        def _():
            for r in blocks:
                hn_ref[r, :] = (h_ref[r, :].astype(F32) + acc_scr[r, :]).astype(BF16)


def fwd_layer(h, hk, w1, k1, w2=None, k2=0):
    b, d = h.shape[1:]
    f = w1.shape[2]
    with_next = w2 is not None
    in_specs = [pl.BlockSpec((None, b, d), lambda j: (hk, 0, 0)), pl.BlockSpec((None, d, TILE), lambda j: (k1, 0, j))]
    out_specs = [pl.BlockSpec((b, TILE), lambda j: (0, j)), pl.BlockSpec((b, TILE), lambda j: (0, j))]
    out_shape = [jax.ShapeDtypeStruct((b, f), F32), jax.ShapeDtypeStruct((b, f), BF16)]
    scratch = [pltpu.VMEM((b, d), BF16)]
    args = [h, w1]
    if with_next:
        in_specs.append(pl.BlockSpec((None, TILE, d), lambda j: (k2, j, 0)))
        out_specs.append(pl.BlockSpec((b, d), lambda j: (0, 0)))
        out_shape.append(jax.ShapeDtypeStruct((b, d), BF16))
        scratch.append(pltpu.VMEM((b, d), F32))
        args.append(w2)
    n_mm = 2 if with_next else 1
    return pl.pallas_call(
        functools.partial(fwd_body, with_next), grid=(f // TILE,), in_specs=in_specs, out_specs=out_specs, out_shape=out_shape,
        scratch_shapes=scratch, compiler_params=params(), name='fwd_next' if with_next else 'fwd_act',
        cost_estimate=cost(2 * n_mm * b * d * f, 4 * n_mm * d * f + 6 * b * f, b * f))(*args)


def head_body(with_grad, loss_scale, a_ref, h_ref, t_ref, w_ref, e_ref, *rest):
    if with_grad:
        q_ref, wire_ref, a_scr, w_scr, acc_scr, elo_scr = rest
    else:
        acc_scr, = rest
    p, j = pl.program_id(0), pl.program_id(1)
    last = pl.num_programs(1) - 1
    blocks = row_blocks(acc_scr.shape[0])

    @pl.when(p == 0)
    def _():
        w = w_ref[...]
        w_lo = w.astype(BF16)
        if with_grad:
            w_scr[j] = w
            a_scr[j] = a_ref[...]

        @pl.when(j == 0)
        def _():
            for r in blocks:
                acc_scr[r, :] = mm(a_ref[r, :], w_lo)

        @pl.when(j > 0)
        def _():
            for r in blocks:
                acc_scr[r, :] += mm(a_ref[r, :], w_lo)

        @pl.when(j == last)
        def _():
            for r in blocks:
                out = (h_ref[r, :].astype(F32) + acc_scr[r, :]).astype(BF16)
                e = loss_scale * (out.astype(F32) - t_ref[r, :].astype(F32))
                e_ref[r, :] = e
                if with_grad:
                    elo_scr[r, :] = e.astype(BF16)

    if with_grad:
        @pl.when(p == 1)
        def _():
            q = w_scr[j] - LEARN_RATE * mm(a_scr[j], elo_scr[...], TN)
            q_ref[...] = q
            wire_ref[...] = q.astype(BF16)


def head(act, h, hk, target, tk, w, wk, wc, hc, half, with_grad, loss_scale):
    b, f = act.shape
    nt = f // TILE
    in_specs = [
        pl.BlockSpec((b, TILE), lambda p, j: (0, j * (1 - p) + (nt - 1) * p)),
        pl.BlockSpec((None, b, half), lambda p, j: (hk, 0, hc)),
        pl.BlockSpec((None, b, half), lambda p, j: (tk, 0, hc)),
        pl.BlockSpec((None, TILE, half), lambda p, j: (wk, j * (1 - p) + (nt - 1) * p, wc)),
    ]
    out_specs = [pl.BlockSpec((b, half), lambda p, j: (0, 0))]
    out_shape = [jax.ShapeDtypeStruct((b, half), F32)]
    scratch = [pltpu.VMEM((b, half), F32)]
    if with_grad:
        out_specs += [pl.BlockSpec((TILE, half), lambda p, j: (j * p, 0))] * 2
        out_shape += [jax.ShapeDtypeStruct((f, half), F32), jax.ShapeDtypeStruct((f, half), BF16)]
        scratch = [pltpu.VMEM((nt, b, TILE), BF16), pltpu.VMEM((nt, TILE, half), F32)] + scratch + [pltpu.VMEM((b, half), BF16)]
    n_mm = 2 if with_grad else 1
    return pl.pallas_call(
        functools.partial(head_body, with_grad, loss_scale), grid=(n_mm, nt), in_specs=in_specs, out_specs=out_specs,
        out_shape=out_shape, scratch_shapes=scratch, name='head_grad' if with_grad else 'head_err',
        compiler_params=pltpu.CompilerParams(dimension_semantics=('arbitrary', 'arbitrary'), vmem_limit_bytes=48 << 20),
        cost_estimate=cost(2 * n_mm * b * half * f, 2 * b * f + 10 * f * half))(act, h, target, w)


def bwd_body(n_e, n_w, with_next, *refs):
    refs = list(refs)
    e_refs = [refs.pop(0) for _ in range(n_e)]
    h_ref, z_ref, a_ref, w1_ref = [refs.pop(0) for _ in range(4)]
    w2_refs = [refs.pop(0) for _ in range(n_w)]
    q1_ref, wire1_ref, q2_ref, wire2_ref = [refs.pop(0) for _ in range(4)]
    if with_next:
        en_ref = refs.pop(0)
    elo_scr, nt_scr, dz_scr = [refs.pop(0) for _ in range(3)]
    if with_next:
        m_scr = refs.pop(0)
    j = pl.program_id(0)
    b, d = h_ref.shape
    blocks = row_blocks(b)
    width = d // n_e
    cols = [slice(k * width, (k + 1) * width) for k in range(n_e)]

    @pl.when(j == 0)
    def _():
        for r in blocks:
            for c, e_ref in zip(cols, e_refs):
                elo_scr[r, c] = e_ref[r, :].astype(BF16)
            x = h_ref[r, :].astype(F32)
            nt_scr[:, r] = (x * inv_rms_of(x)).T.astype(BF16)
            if with_next:
                m_scr[r, :] = jnp.zeros((ROWS, d), F32)

    w1 = w1_ref[...].astype(BF16)
    if n_w == 1:
        w2 = w2_refs[0][...].astype(BF16)
    else:
        w2 = jnp.concatenate([w[...].astype(BF16) for w in w2_refs], axis=1)
    for r in blocks:
        u = mm(elo_scr[r, :], w2, NT)
        dz = (u * gelu_slope(z_ref[r, :])).astype(BF16)
        dz_scr[r, :] = dz
        if with_next:
            m_scr[r, :] += mm(dz, w1, NT)
    q1 = w1_ref[...] - LEARN_RATE * mm(nt_scr[...], dz_scr[...])
    q1_ref[...] = q1
    wire1_ref[...] = q1.astype(BF16)
    q2 = w2_refs[-1][...] - LEARN_RATE * mm(a_ref[...], elo_scr[:, cols[-1]], TN)
    q2_ref[...] = q2
    wire2_ref[...] = q2.astype(BF16)

    if with_next:
        @pl.when(j == pl.num_programs(0) - 1)
        def _():
            for r in blocks:
                x = h_ref[r, :].astype(F32)
                s = inv_rms_of(x)
                n = x * s
                m = m_scr[r, :]
                step = s * (m - n * jnp.mean(m * n, axis=-1, keepdims=True))
                for c, e_ref in zip(cols, e_refs):
                    en_ref[r, c] = e_ref[r, :] + step[:, c]


def bwd_layer(e_list, h, hk, z, a, w1, k1, w2_list, with_next):
    b, d = h.shape[1:]
    f = z.shape[1]
    width = d // len(e_list)
    col_of = [c for _, _, c in w2_list]
    in_specs = [pl.BlockSpec((b, width), lambda j: (0, 0)) for _ in e_list]
    in_specs += [pl.BlockSpec((None, b, d), lambda j: (hk, 0, 0)), pl.BlockSpec((b, TILE), lambda j: (0, j)),
                 pl.BlockSpec((b, TILE), lambda j: (0, j)), pl.BlockSpec((None, d, TILE), lambda j: (k1, 0, j))]
    for _, k, c in w2_list:
        in_specs.append(pl.BlockSpec((None, TILE, width), functools.partial(lambda k, c, j: (k, j, c), k, c)))
    out_specs = [pl.BlockSpec((d, TILE), lambda j: (0, j))] * 2 + [pl.BlockSpec((TILE, width), lambda j: (j, 0))] * 2
    out_shape = [jax.ShapeDtypeStruct((d, f), F32), jax.ShapeDtypeStruct((d, f), BF16),
                 jax.ShapeDtypeStruct((f, width), F32), jax.ShapeDtypeStruct((f, width), BF16)]
    scratch = [pltpu.VMEM((b, d), BF16), pltpu.VMEM((d, b), BF16), pltpu.VMEM((b, TILE), BF16)]
    if with_next:
        out_specs.append(pl.BlockSpec((b, d), lambda j: (0, 0)))
        out_shape.append(jax.ShapeDtypeStruct((b, d), F32))
        scratch.append(pltpu.VMEM((b, d), F32))
    n_mm = 4 if with_next else 3
    return pl.pallas_call(
        functools.partial(bwd_body, len(e_list), len(w2_list), with_next), grid=(f // TILE,), in_specs=in_specs,
        out_specs=out_specs, out_shape=out_shape, scratch_shapes=scratch, compiler_params=params(56),
        name='bwd_last' if len(e_list) > 1 else 'bwd_mid' if with_next else 'bwd_first',
        cost_estimate=cost(2 * n_mm * b * d * f, 20 * d * f + 6 * b * f, b * f))(
            *e_list, h, z, a, w1, *[w for w, _, _ in w2_list])


def mix_vals(own, prev, nxt, row):
    row = row.astype(F32)
    return (own + prev.astype(F32) + nxt.astype(F32) + row + row) / 5.0


def place_body(n_alias, own_ref, prev_ref, nxt_ref, row_ref, *rest):
    out_ref = rest[n_alias]
    out_ref[...] = mix_vals(own_ref[...], prev_ref[...], nxt_ref[...], row_ref[...])


def place(stack, shape, layer, col, own, recv):
    r, c = own.shape
    tr = r // 4
    spec = pl.BlockSpec((tr, c), lambda i: (i, 0))
    args = [own, *recv]
    in_specs = [spec] * 4
    aliases = {}
    if stack is not None:
        args.append(stack)
        in_specs.append(pl.BlockSpec(memory_space=pl.ANY))
        aliases = {4: 0}
    return pl.pallas_call(
        functools.partial(place_body, len(aliases)), grid=(4,), in_specs=in_specs,
        out_specs=pl.BlockSpec((None, tr, c), lambda i: (layer, i, col)), out_shape=jax.ShapeDtypeStruct(shape, F32),
        input_output_aliases=aliases, compiler_params=params(), name='place',
        cost_estimate=cost(5 * r * c, 14 * r * c))(*args)


def solution(mesh):
    n_rows = mesh.shape['row']
    n_cols = mesh.shape['col']
    from_col_prev = [(i, (i + 1) % n_cols) for i in range(n_cols)]
    from_col_next = [(i, (i - 1) % n_cols) for i in range(n_cols)]
    from_row = [(i, (i + 1) % n_rows) for i in range(n_rows)]

    def after(value, *others):
        return lax.optimization_barrier((value,) + others)[0]

    def send(wire):
        row = lax.ppermute(wire, 'row', from_row)
        return lax.ppermute(wire, 'col', from_col_prev), lax.ppermute(wire, 'col', from_col_next), row

    def device_fn(w_one, w_two, inputs, targets):
        n_layers, d, f = w_one.shape[2:]
        last = n_layers - 1
        half = d // 2
        n_steps, b = inputs.shape[2:4]
        loss_scale = 2.0 / (b * d)
        stack_one, stack_two = w_one[0, 0], w_two[0, 0]
        x_all, t_all = inputs[0, 0], targets[0, 0]
        one = [(stack_one, k) for k in range(n_layers)]
        two = [(stack_two, k) for k in range(last)]
        halves = [(stack_two, last, 0), (stack_two, last, 1)]
        for step in range(n_steps):
            hidden = [(x_all, step)]
            saved = []
            for l in range(last):
                z, a, nxt = fwd_layer(*hidden[l], *one[l], *two[l])
                saved.append((z, a))
                hidden.append((nxt[None], 0))
            saved.append(fwd_layer(*hidden[last], *one[last]))
            recvs, names, own, outs = [], [], {}, {}
            final = step == n_steps - 1

            def settle(k):
                name = names[k]
                if name[0] == 'one':
                    outs['one'] = place(outs.get('one'), stack_one.shape, name[1], 0, own[name], recvs[k])
                else:
                    layer, col = (last, int(name[1])) if name[0] == 'h' else (name[1], 0)
                    outs['two'] = place(outs.get('two'), stack_two.shape, layer, col, own[name], recvs[k])

            def push(name, q, wire, gate=None):
                if gate is not None and final:
                    settle(gate)
                    kinds = sorted(outs)
                    wire, *vals = lax.optimization_barrier((wire, *recvs[gate], *[outs[k] for k in kinds]))
                    outs.update(zip(kinds, vals[3:]))
                elif gate is not None:
                    wire = after(wire, *recvs[gate])
                recvs.append(send(wire))
                names.append(name)
                own[name] = q

            act = saved[last][1]
            e0, q, wire = head(act, *hidden[last], t_all, step, *halves[0], 0, half, True, loss_scale)
            push('h0', q, wire)
            e1, = head(act, *hidden[last], t_all, step, *halves[1], 1, half, False, loss_scale)
            e_list = [e0, e1]
            ready = {}
            for l in reversed(range(n_layers)):
                w2_list = halves if l == last else [two[l] + (0,)]
                res = bwd_layer(e_list, *hidden[l], *saved[l], *one[l], w2_list, l > 0)
                ready['one', l] = res[0:2]
                ready['h1' if l == last else ('two', l)] = res[2:4]
                if l > 0:
                    e_list = [res[4]]
            push(('one', last), *ready['one', last])
            early = ('one', last - 1)
            order = [early] + [(kind, l) for l in range(last) for kind in ('one', 'two') if (kind, l) != early] + ['h1']
            for name in order:
                push(name, *ready[name], gate=len(recvs) - 2)
            if not final:
                mixed = {name: mix_vals(own[name], *recv)[None] for name, recv in zip(names, recvs)}
                one = [(mixed['one', l], 0) for l in range(n_layers)]
                two = [(mixed['two', l], 0) for l in range(last)]
                halves = [(mixed['h0'], 0, 0), (mixed['h1'], 0, 0)]
        for k in range(len(names) - 2, len(names)):
            settle(k)
        return outs['one'][None, None], outs['two'][None, None]

    grid_spec = P('row', 'col')
    return jax.shard_map(device_fn, mesh=mesh, in_specs=(grid_spec, grid_spec, grid_spec, grid_spec), out_specs=(grid_spec, grid_spec), check_vma=False)
```

```python
import functools

import jax
import jax.numpy as jnp
from jax import lax
from jax.experimental import pallas as pl
from jax.experimental.pallas import tpu as pltpu
from jax.sharding import PartitionSpec as P


LEARN_RATE = 1.5
NORM_EPS = 1e-6
GELU_C = 0.7978845608028654
GELU_K = 0.044715
TILE = 512
ROWS = 1024
F32 = jnp.float32
BF16 = jnp.bfloat16


def gelu_value(z):
    tanh_inner = jnp.tanh(z * (GELU_C + (GELU_C * GELU_K) * (z * z)))
    half = 0.5 * z
    return half + half * tanh_inner


def gelu_both(z):
    sq = z * z
    tanh_inner = jnp.tanh(z * (GELU_C + (GELU_C * GELU_K) * sq))
    half = 0.5 * z
    value = half + half * tanh_inner
    slope = (0.5 + 0.5 * tanh_inner) + (half * (1.0 - tanh_inner * tanh_inner)) * (GELU_C + (3.0 * GELU_C * GELU_K) * sq)
    return value, slope


def mm(a, b, dims=((1,), (0,))):
    return lax.dot_general(a, b, (dims, ((), ())), preferred_element_type=F32)


NT = ((1,), (1,))
TN = ((0,), (0,))


def inv_rms_of(x):
    return lax.rsqrt(jnp.mean(x * x, axis=-1, keepdims=True) + NORM_EPS)


def norm_back(x, m):
    inv = inv_rms_of(x)
    n = x * inv
    return inv * (m - n * jnp.mean(m * n, axis=-1, keepdims=True))


def row_blocks(n):
    return [slice(k, k + ROWS) for k in range(0, n, ROWS)]


def params(mib=48):
    return pltpu.CompilerParams(dimension_semantics=('arbitrary',), vmem_limit_bytes=mib << 20)


def cost(flops, nbytes, trans=0):
    return pl.CostEstimate(flops=flops, bytes_accessed=nbytes, transcendentals=trans)


def fwd_body(h_ref, w1_ref, w2_ref, hn_ref, n_scr, acc_scr):
    j = pl.program_id(0)
    blocks = row_blocks(h_ref.shape[0])

    @pl.when(j == 0)
    def _():
        for r in blocks:
            x = h_ref[r, :].astype(F32)
            n_scr[r, :] = (x * inv_rms_of(x)).astype(BF16)
            acc_scr[r, :] = jnp.zeros((ROWS, acc_scr.shape[1]), F32)

    w1 = w1_ref[...].astype(BF16)
    w2 = w2_ref[...].astype(BF16)
    for r in blocks:
        a = gelu_value(mm(n_scr[r, :], w1)).astype(BF16)
        acc_scr[r, :] += mm(a, w2)

    @pl.when(j == pl.num_programs(0) - 1)
    def _():
        for r in blocks:
            hn_ref[r, :] = (h_ref[r, :].astype(F32) + acc_scr[r, :]).astype(BF16)


def fwd_layer(h, hk, w1, k1, w2, k2):
    b, d = h.shape[1:]
    f = w1.shape[2]
    return pl.pallas_call(
        fwd_body, grid=(f // TILE,), name='fwd',
        in_specs=[pl.BlockSpec((None, b, d), lambda j: (hk, 0, 0)), pl.BlockSpec((None, d, TILE), lambda j: (k1, 0, j)),
                  pl.BlockSpec((None, TILE, d), lambda j: (k2, j, 0))],
        out_specs=pl.BlockSpec((b, d), lambda j: (0, 0)), out_shape=jax.ShapeDtypeStruct((b, d), BF16),
        scratch_shapes=[pltpu.VMEM((b, d), BF16), pltpu.VMEM((b, d), F32)], compiler_params=params(),
        cost_estimate=cost(4 * b * d * f, 8 * d * f + 4 * b * d, b * f))(h, w1, w2)


def chain_body(n_fwd, nt, mixing, loss_scale, *refs):
    refs = list(refs)
    h_ref, hist_ref = refs.pop(0), None
    w1f_ref = refs.pop(0)
    w2f_refs = [refs.pop(0) for _ in range(4 if mixing else 1)]
    t_ref, w1h_ref, w2h_ref = [refs.pop(0) for _ in range(3)]
    hist_ref, a_ref, e_ref, q_ref, wire_ref = [refs.pop(0) for _ in range(5)]
    if mixing:
        p_ref = refs.pop(0)
    h_scr, n_scr, acc_scr, a_scr, w_scr, elo_scr = refs
    i = pl.program_id(0)
    j = lax.rem(i, nt)
    in_fwd = i < n_fwd * nt
    in_head = (i >= n_fwd * nt) & (i < (n_fwd + 1) * nt)
    b = h_ref.shape[0]
    half = e_ref.shape[1]
    blocks = row_blocks(b)

    @pl.when(i == 0)
    def _():
        h_scr[...] = h_ref[...]

    @pl.when((j == 0) & (i <= n_fwd * nt))
    def _():
        for r in blocks:
            x = h_scr[r, :].astype(F32)
            n_scr[r, :] = (x * inv_rms_of(x)).astype(BF16)
        acc_scr[...] = jnp.zeros_like(acc_scr)

    @pl.when(in_fwd)
    def _():
        w1 = w1f_ref[...].astype(BF16)
        if mixing:
            w2 = mix_vals(*[w[...] for w in w2f_refs])
            p_ref[...] = w2
        else:
            w2 = w2f_refs[0][...]
        w2 = w2.astype(BF16)
        for r in blocks:
            a = gelu_value(mm(n_scr[r, :], w1)).astype(BF16)
            acc_scr[r, :] += mm(a, w2)

    @pl.when(in_fwd & (j == nt - 1))
    def _():
        for r in blocks:
            out = (h_scr[r, :].astype(F32) + acc_scr[r, :]).astype(BF16)
            h_scr[r, :] = out
            hist_ref[r, :] = out

    @pl.when(in_head)
    def _():
        w1 = w1h_ref[...].astype(BF16)
        w2 = w2h_ref[...]
        w_scr[j] = w2
        w2 = w2.astype(BF16)
        for r in blocks:
            a = gelu_value(mm(n_scr[r, :], w1)).astype(BF16)
            a_scr[j, r, :] = a
            a_ref[r, :] = a
            acc_scr[r, :half] += mm(a, w2)

    @pl.when(in_head & (j == nt - 1))
    def _():
        for r in blocks:
            out = (h_scr[r, :half].astype(F32) + acc_scr[r, :half]).astype(BF16)
            e = loss_scale * (out.astype(F32) - t_ref[r, :].astype(F32))
            e_ref[r, :] = e
            elo_scr[r, :] = e.astype(BF16)

    @pl.when(i >= (n_fwd + 1) * nt)
    def _():
        q = w_scr[j] - LEARN_RATE * mm(a_scr[j], elo_scr[...], TN)
        q_ref[...] = q
        wire_ref[...] = q.astype(BF16)


def chain(n_fwd, h, hk, target, tk, w1f, k1f, w2f, k2f, w1h, k1h, w2h, k2h, half, loss_scale):
    b, d = h.shape[1:]
    f = w1f.shape[2]
    nt = f // TILE
    mixing = isinstance(w2f, tuple)
    n_steps = n_fwd * nt

    def f_layer(i):
        return jnp.minimum(i, n_steps - 1) // nt

    def f_tile(i):
        return jnp.minimum(i, n_steps - 1) % nt

    def h_tile(i):
        return jnp.clip(i - n_steps, 0, nt - 1)

    def g_tile(i):
        return jnp.maximum(i - n_steps - nt, 0)

    in_specs = [pl.BlockSpec((None, b, d), lambda i: (hk, 0, 0)),
                pl.BlockSpec((None, d, TILE), lambda i: (k1f + f_layer(i), 0, f_tile(i)))]
    if mixing:
        in_specs += [pl.BlockSpec((TILE, d), lambda i: (f_tile(i), 0))] * 4
    else:
        in_specs.append(pl.BlockSpec((None, TILE, d), lambda i: (k2f + f_layer(i), f_tile(i), 0)))
    in_specs += [pl.BlockSpec((None, b, half), lambda i: (tk, 0, 0)), pl.BlockSpec((None, d, TILE), lambda i: (k1h, 0, h_tile(i))),
                 pl.BlockSpec((None, TILE, half), lambda i: (k2h, h_tile(i), 0))]
    out_specs = [pl.BlockSpec((None, b, d), lambda i: (f_layer(i), 0, 0)), pl.BlockSpec((b, TILE), lambda i: (0, h_tile(i))),
                 pl.BlockSpec((b, half), lambda i: (0, 0))] + [pl.BlockSpec((TILE, half), lambda i: (g_tile(i), 0))] * 2
    out_shape = [jax.ShapeDtypeStruct((n_fwd, b, d), BF16), jax.ShapeDtypeStruct((b, f), BF16), jax.ShapeDtypeStruct((b, half), F32),
                 jax.ShapeDtypeStruct((f, half), F32), jax.ShapeDtypeStruct((f, half), BF16)]
    if mixing:
        out_specs.append(pl.BlockSpec((TILE, d), lambda i: (f_tile(i), 0)))
        out_shape.append(jax.ShapeDtypeStruct((f, d), F32))
    return pl.pallas_call(
        functools.partial(chain_body, n_fwd, nt, mixing, loss_scale), grid=((n_fwd + 2) * nt,), name='chain',
        in_specs=in_specs, out_specs=out_specs, out_shape=out_shape,
        scratch_shapes=[pltpu.VMEM((b, d), BF16), pltpu.VMEM((b, d), BF16), pltpu.VMEM((b, d), F32), pltpu.VMEM((nt, b, TILE), BF16),
                        pltpu.VMEM((nt, TILE, half), F32), pltpu.VMEM((b, half), BF16)],
        compiler_params=params(),
        cost_estimate=cost(2 * b * f * (2 * n_fwd * d + d + 2 * half), 8 * n_fwd * d * f + 4 * d * f + 2 * b * f + 10 * f * half, (n_fwd + 1) * b * f))(
            h, w1f, *(w2f if mixing else (w2f,)), target, w1h, w2h)


def tail_body(nt, mixing, loss_scale, *refs):
    refs = list(refs)
    a_ref, h_ref, hc_ref, t_ref, e0_ref, w1_ref, w20_ref = [refs.pop(0) for _ in range(7)]
    w21_refs = [refs.pop(0) for _ in range(4 if mixing else 1)]
    e1_ref, dz_ref, q_ref, wire_ref = [refs.pop(0) for _ in range(4)]
    if mixing:
        p_ref = refs.pop(0)
    n_scr, acc_scr, w2_scr, elo_scr = refs
    i = pl.program_id(0)
    j = lax.rem(i, nt)
    blocks = row_blocks(h_ref.shape[0])
    half = e0_ref.shape[1]

    @pl.when(i == 0)
    def _():
        acc_scr[...] = jnp.zeros_like(acc_scr)
        for r in blocks:
            x = h_ref[r, :].astype(F32)
            n_scr[r, :] = (x * inv_rms_of(x)).astype(BF16)

    @pl.when(i < nt)
    def _():
        if mixing:
            w2 = mix_vals(*[w[...] for w in w21_refs])
            p_ref[...] = w2
        else:
            w2 = w21_refs[0][...]
        w2 = w2.astype(BF16)
        w2_scr[j, :, :half] = w20_ref[...].astype(BF16)
        w2_scr[j, :, half:] = w2
        acc_scr[...] += mm(a_ref[...], w2)

    @pl.when(i == nt - 1)
    def _():
        for r in blocks:
            out = (hc_ref[r, :].astype(F32) + acc_scr[r, :]).astype(BF16)
            e = loss_scale * (out.astype(F32) - t_ref[r, :].astype(F32))
            e1_ref[r, :] = e
            elo_scr[r, :half] = e0_ref[r, :].astype(BF16)
            elo_scr[r, half:] = e.astype(BF16)

    @pl.when(i >= nt)
    def _():
        w1 = w1_ref[...]
        w1_lo = w1.astype(BF16)
        for r in blocks:
            _, slope = gelu_both(mm(n_scr[r, :], w1_lo))
            dz_ref[r, :] = (mm(elo_scr[r, :], w2_scr[j], NT) * slope).astype(BF16)
        q = w1 - LEARN_RATE * mm(n_scr[...], dz_ref[...], TN)
        q_ref[...] = q
        wire_ref[...] = q.astype(BF16)


def tail(act, h, hk, target, tk, e0, w1, k1, w20, k20, w21, k21, c21, half, loss_scale):
    b, d = h.shape[1:]
    f = w1.shape[2]
    nt = f // TILE
    mixing = isinstance(w21, tuple)

    def p_tile(i):
        return jnp.minimum(i, nt - 1)

    def g_tile(i):
        return jnp.maximum(i - nt, 0)

    in_specs = [pl.BlockSpec((b, TILE), lambda i: (0, p_tile(i))), pl.BlockSpec((None, b, d), lambda i: (hk, 0, 0)),
                pl.BlockSpec((None, b, half), lambda i: (hk, 0, 1)), pl.BlockSpec((None, b, half), lambda i: (tk, 0, 1)),
                pl.BlockSpec((b, half), lambda i: (0, 0)), pl.BlockSpec((None, d, TILE), lambda i: (k1, 0, g_tile(i))),
                pl.BlockSpec((None, TILE, half), lambda i: (k20, p_tile(i), 0))]
    if mixing:
        in_specs += [pl.BlockSpec((TILE, half), lambda i: (p_tile(i), 0))] * 4
    else:
        in_specs.append(pl.BlockSpec((None, TILE, half), lambda i: (k21, p_tile(i), c21)))
    out_specs = [pl.BlockSpec((b, half), lambda i: (0, 0)), pl.BlockSpec((b, TILE), lambda i: (0, g_tile(i)))]
    out_specs += [pl.BlockSpec((d, TILE), lambda i: (0, g_tile(i)))] * 2
    out_shape = [jax.ShapeDtypeStruct((b, half), F32), jax.ShapeDtypeStruct((b, f), BF16), jax.ShapeDtypeStruct((d, f), F32),
                 jax.ShapeDtypeStruct((d, f), BF16)]
    if mixing:
        out_specs.append(pl.BlockSpec((TILE, half), lambda i: (p_tile(i), 0)))
        out_shape.append(jax.ShapeDtypeStruct((f, half), F32))
    return pl.pallas_call(
        functools.partial(tail_body, nt, mixing, loss_scale), grid=(2 * nt,), name='tail', in_specs=in_specs, out_specs=out_specs,
        out_shape=out_shape,
        scratch_shapes=[pltpu.VMEM((b, d), BF16), pltpu.VMEM((b, half), F32), pltpu.VMEM((nt, TILE, d), BF16), pltpu.VMEM((b, d), BF16)],
        compiler_params=params(),
        cost_estimate=cost(2 * b * f * (3 * d + half), 10 * d * f + 8 * f * half + 4 * b * f, b * f))(
            act, h, h, target, e0, w1, w20, *(w21 if mixing else (w21,)))


def last_body(a_ref, dz_ref, h_ref, e0_ref, e1_ref, w1_ref, w2_ref, q_ref, wire_ref, en_ref, m_scr, elo_scr):
    j = pl.program_id(0)
    blocks = row_blocks(h_ref.shape[0])
    half = e0_ref.shape[1]

    @pl.when(j == 0)
    def _():
        m_scr[...] = jnp.zeros_like(m_scr)
        elo_scr[...] = e1_ref[...].astype(BF16)

    m_scr[...] += mm(dz_ref[...], w1_ref[...].astype(BF16), NT)
    q = w2_ref[...] - LEARN_RATE * mm(a_ref[...], elo_scr[...], TN)
    q_ref[...] = q
    wire_ref[...] = q.astype(BF16)

    @pl.when(j == pl.num_programs(0) - 1)
    def _():
        for r in blocks:
            step = norm_back(h_ref[r, :].astype(F32), m_scr[r, :])
            en_ref[r, :half] = e0_ref[r, :] + step[:, :half]
            en_ref[r, half:] = e1_ref[r, :] + step[:, half:]


def bwd_last(act, dz, h, hk, e0, e1, w1, k1, w2, k2, c2, half):
    b, d = h.shape[1:]
    f = w1.shape[2]
    return pl.pallas_call(
        last_body, grid=(f // TILE,), name='bwd_last',
        in_specs=[pl.BlockSpec((b, TILE), lambda j: (0, j))] * 2 + [pl.BlockSpec((None, b, d), lambda j: (hk, 0, 0))]
        + [pl.BlockSpec((b, half), lambda j: (0, 0))] * 2
        + [pl.BlockSpec((None, d, TILE), lambda j: (k1, 0, j)), pl.BlockSpec((None, TILE, half), lambda j: (k2, j, c2))],
        out_specs=[pl.BlockSpec((TILE, half), lambda j: (j, 0))] * 2 + [pl.BlockSpec((b, d), lambda j: (0, 0))],
        out_shape=[jax.ShapeDtypeStruct((f, half), F32), jax.ShapeDtypeStruct((f, half), BF16), jax.ShapeDtypeStruct((b, d), F32)],
        scratch_shapes=[pltpu.VMEM((b, d), F32), pltpu.VMEM((b, half), BF16)], compiler_params=params(),
        cost_estimate=cost(2 * b * f * (d + half), 4 * d * f + 10 * f * half + 4 * b * f))(act, dz, h, e0, e1, w1, w2)


def bwd_body(with_next, e_ref, h_ref, w1_ref, w2_ref, q1_ref, wire1_ref, q2_ref, wire2_ref, *rest):
    if with_next:
        en_ref, elo_scr, n_scr, a_scr, dz_scr, m_scr = rest
    else:
        elo_scr, n_scr, a_scr, dz_scr = rest
    j = pl.program_id(0)
    blocks = row_blocks(h_ref.shape[0])

    @pl.when(j == 0)
    def _():
        for r in blocks:
            elo_scr[r, :] = e_ref[r, :].astype(BF16)
            x = h_ref[r, :].astype(F32)
            n_scr[r, :] = (x * inv_rms_of(x)).astype(BF16)
        if with_next:
            m_scr[...] = jnp.zeros_like(m_scr)

    w1 = w1_ref[...].astype(BF16)
    w2 = w2_ref[...].astype(BF16)
    for r in blocks:
        value, slope = gelu_both(mm(n_scr[r, :], w1))
        a_scr[r, :] = value.astype(BF16)
        dz = (mm(elo_scr[r, :], w2, NT) * slope).astype(BF16)
        dz_scr[r, :] = dz
        if with_next:
            m_scr[r, :] += mm(dz, w1, NT)
    q1 = w1_ref[...] - LEARN_RATE * mm(n_scr[...], dz_scr[...], TN)
    q1_ref[...] = q1
    wire1_ref[...] = q1.astype(BF16)
    q2 = w2_ref[...] - LEARN_RATE * mm(a_scr[...], elo_scr[...], TN)
    q2_ref[...] = q2
    wire2_ref[...] = q2.astype(BF16)

    if with_next:
        @pl.when(j == pl.num_programs(0) - 1)
        def _():
            for r in blocks:
                en_ref[r, :] = e_ref[r, :] + norm_back(h_ref[r, :].astype(F32), m_scr[r, :])


def bwd_layer(e, h, hk, w1, k1, w2, k2, with_next):
    b, d = h.shape[1:]
    f = w1.shape[2]
    out_specs = [pl.BlockSpec((d, TILE), lambda j: (0, j))] * 2 + [pl.BlockSpec((TILE, d), lambda j: (j, 0))] * 2
    out_shape = [jax.ShapeDtypeStruct((d, f), F32), jax.ShapeDtypeStruct((d, f), BF16),
                 jax.ShapeDtypeStruct((f, d), F32), jax.ShapeDtypeStruct((f, d), BF16)]
    scratch = [pltpu.VMEM((b, d), BF16), pltpu.VMEM((b, d), BF16), pltpu.VMEM((b, TILE), BF16), pltpu.VMEM((b, TILE), BF16)]
    if with_next:
        out_specs.append(pl.BlockSpec((b, d), lambda j: (0, 0)))
        out_shape.append(jax.ShapeDtypeStruct((b, d), F32))
        scratch.append(pltpu.VMEM((b, d), F32))
    n_mm = 5 if with_next else 4
    return pl.pallas_call(
        functools.partial(bwd_body, with_next), grid=(f // TILE,), name='bwd_mid' if with_next else 'bwd_first',
        in_specs=[pl.BlockSpec((b, d), lambda j: (0, 0)), pl.BlockSpec((None, b, d), lambda j: (hk, 0, 0)),
                  pl.BlockSpec((None, d, TILE), lambda j: (k1, 0, j)), pl.BlockSpec((None, TILE, d), lambda j: (k2, j, 0))],
        out_specs=out_specs, out_shape=out_shape, scratch_shapes=scratch, compiler_params=params(),
        cost_estimate=cost(2 * n_mm * b * d * f, 20 * d * f, b * f))(e, h, w1, w2)


def mix_vals(own, prev, nxt, row):
    row = row.astype(F32)
    return (own + prev.astype(F32) + nxt.astype(F32) + row + row) / 5.0


def place_body(n_alias, own_ref, prev_ref, nxt_ref, row_ref, *rest):
    out_ref = rest[n_alias]
    out_ref[...] = mix_vals(own_ref[...], prev_ref[...], nxt_ref[...], row_ref[...])


def place(stack, shape, layer, col, own, recv):
    r, c = own.shape
    tr = r // 4
    spec = pl.BlockSpec((tr, c), lambda i: (i, 0))
    args = [own, *recv]
    in_specs = [spec] * 4
    aliases = {}
    if stack is not None:
        args.append(stack)
        in_specs.append(pl.BlockSpec(memory_space=pl.ANY))
        aliases = {4: 0}
    return pl.pallas_call(
        functools.partial(place_body, len(aliases)), grid=(4,), in_specs=in_specs,
        out_specs=pl.BlockSpec((None, tr, c), lambda i: (layer, i, col)), out_shape=jax.ShapeDtypeStruct(shape, F32),
        input_output_aliases=aliases, compiler_params=params(), name='place',
        cost_estimate=cost(5 * r * c, 14 * r * c))(*args)


def solution(mesh):
    n_rows = mesh.shape['row']
    n_cols = mesh.shape['col']
    from_col_prev = [(i, (i + 1) % n_cols) for i in range(n_cols)]
    from_col_next = [(i, (i - 1) % n_cols) for i in range(n_cols)]
    from_row = [(i, (i + 1) % n_rows) for i in range(n_rows)]

    def after(value, *others):
        return lax.optimization_barrier((value,) + others)[0]

    def send(wire):
        row = lax.ppermute(wire, 'row', from_row)
        prev = lax.ppermute(wire, 'col', from_col_prev)
        nxt = lax.ppermute(wire, 'col', from_col_next)
        return prev, nxt, row

    def device_fn(w_one, w_two, inputs, targets):
        n_layers, d, _ = w_one.shape[2:]
        last = n_layers - 1
        half = d // 2
        n_steps, b = inputs.shape[2:4]
        loss_scale = 2.0 / (b * d)
        stack_one, stack_two = w_one[0, 0], w_two[0, 0]
        x_all, t_all = inputs[0, 0], targets[0, 0]
        one = [(stack_one, k) for k in range(n_layers)]
        two = [(stack_two, k) for k in range(last)]
        halves = [(stack_two, last), (stack_two, last, 1)]
        for step in range(n_steps):
            recvs, names, own, outs = [], [], {}, {}
            final = step == n_steps - 1

            def settle(k):
                name = names[k]
                if name[0] == 'one':
                    outs['one'] = place(outs.get('one'), stack_one.shape, name[1], 0, own[name], recvs[k])
                else:
                    layer, col = (last, int(name[1])) if name[0] == 'h' else (name[1], 0)
                    outs['two'] = place(outs.get('two'), stack_two.shape, layer, col, own[name], recvs[k])

            def push(name, q, wire, gate=None):
                if gate is not None and final:
                    settle(gate)
                    kinds = sorted(outs)
                    wire, *vals = lax.optimization_barrier((wire, *recvs[gate], *[outs[k] for k in kinds]))
                    outs.update(zip(kinds, vals[3:]))
                elif gate is not None:
                    wire = after(wire, *recvs[gate])
                recvs.append(send(wire))
                names.append(name)
                own[name] = q

            hidden = [(x_all, step)]
            if step == 0:
                hist, act, e0, q, wire = chain(last, *hidden[0], t_all, step, stack_one, 0, stack_two, 0, stack_one, last, stack_two, last, half, loss_scale)
                hidden += [(hist, l) for l in range(last)]
            else:
                for l in range(last - 1):
                    hidden.append((fwd_layer(*hidden[l], *one[l], *two[l])[None], 0))
                hist, act, e0, q, wire, mixed_two = chain(1, *hidden[last - 1], t_all, step, *one[last - 1], two[last - 1], 0, *one[last], *halves[0], half, loss_scale)
                two[last - 1] = (mixed_two[None], 0)
                hidden.append((hist, 0))
            push('h0', q, wire)
            res = tail(act, *hidden[last], t_all, step, e0, *one[last], *halves[0], *halves[1], half, loss_scale)
            e1, dz = res[:2]
            push(('one', last), *res[2:4])
            if step > 0:
                halves[1] = (res[4][None], 0, 0)
            ready = {}
            q, wire, err = bwd_last(act, dz, *hidden[last], e0, e1, *one[last], *halves[1], half)
            ready['h1'] = (q, wire)
            for l in reversed(range(last)):
                res = bwd_layer(err, *hidden[l], *one[l], *two[l], l > 0)
                ready['one', l], ready['two', l] = res[0:2], res[2:4]
                if l > 0:
                    err = res[4]
            early = ('one', last - 1)
            order = [early] + [(kind, l) for l in range(last) for kind in ('one', 'two') if (kind, l) != early] + ['h1']
            for name in order:
                push(name, *ready[name], gate=len(recvs) - 2)
            if not final:
                parts = {name: (own[name], *recv) for name, recv in zip(names, recvs)}
                deferred = ('h1', ('two', last - 1))
                mixed = {name: mix_vals(*vals)[None] for name, vals in parts.items() if name not in deferred}
                one = [(mixed['one', l], 0) for l in range(n_layers)]
                two = [(mixed['two', l], 0) for l in range(last - 1)] + [parts['two', last - 1]]
                halves = [(mixed['h0'], 0), (parts['h1'], 0, 0)]
        for k in range(len(names) - 2, len(names)):
            settle(k)
        return outs['one'][None, None], outs['two'][None, None]

    grid_spec = P('row', 'col')
    return jax.shard_map(device_fn, mesh=mesh, in_specs=(grid_spec, grid_spec, grid_spec, grid_spec), out_specs=(grid_spec, grid_spec), check_vma=False)
```

```python
import functools

import jax
import jax.numpy as jnp
from jax import lax
from jax.experimental import pallas as pl
from jax.experimental.pallas import tpu as pltpu
from jax.sharding import PartitionSpec as P


LEARN_RATE = 1.5
NORM_EPS = 1e-6
GELU_C = 0.7978845608028654
GELU_K = 0.044715
TILE = 512
ROWS = 1024
THIN = 128
F32 = jnp.float32
BF16 = jnp.bfloat16


def gelu_value(z):
    tanh_inner = jnp.tanh(z * (GELU_C + (GELU_C * GELU_K) * (z * z)))
    half = 0.5 * z
    return half + half * tanh_inner


def gelu_both(z):
    sq = z * z
    tanh_inner = jnp.tanh(z * (GELU_C + (GELU_C * GELU_K) * sq))
    half = 0.5 * z
    value = half + half * tanh_inner
    slope = (0.5 + 0.5 * tanh_inner) + (half * (1.0 - tanh_inner * tanh_inner)) * (GELU_C + (3.0 * GELU_C * GELU_K) * sq)
    return value, slope


def mm(a, b, dims=((1,), (0,))):
    return lax.dot_general(a, b, (dims, ((), ())), preferred_element_type=F32)


NT = ((1,), (1,))
TN = ((0,), (0,))


def inv_rms_of(x):
    return lax.rsqrt(jnp.mean(x * x, axis=-1, keepdims=True) + NORM_EPS)


def norm_back(x, m):
    inv = inv_rms_of(x)
    n = x * inv
    return inv * (m - n * jnp.mean(m * n, axis=-1, keepdims=True))


def row_blocks(n, rows=ROWS):
    return [slice(k, k + rows) for k in range(0, n, rows)]


def params(mib=62):
    return pltpu.CompilerParams(dimension_semantics=('arbitrary',), vmem_limit_bytes=mib << 20)


def cost(flops, nbytes, trans=0):
    return pl.CostEstimate(flops=flops, bytes_accessed=nbytes, transcendentals=trans)


def fwd_body(h_ref, w1_ref, w2_ref, hn_ref, n_scr, acc_scr):
    j = pl.program_id(0)
    blocks = row_blocks(h_ref.shape[0])
    thin = row_blocks(h_ref.shape[0], THIN)

    @pl.when(j == 0)
    def _():
        for r in thin:
            x = h_ref[r, :].astype(F32)
            n_scr[r, :] = (x * inv_rms_of(x)).astype(BF16)
        acc_scr[...] = jnp.zeros_like(acc_scr)

    w1 = w1_ref[...].astype(BF16)
    w2 = w2_ref[...].astype(BF16)
    for r in blocks:
        a = gelu_value(mm(n_scr[r, :], w1)).astype(BF16)
        acc_scr[r, :] += mm(a, w2)

    @pl.when(j == pl.num_programs(0) - 1)
    def _():
        for r in thin:
            hn_ref[r, :] = (h_ref[r, :].astype(F32) + acc_scr[r, :]).astype(BF16)


def fwd_layer(h, hk, w1, k1, w2, k2):
    b, d = h.shape[1:]
    f = w1.shape[2]
    return pl.pallas_call(
        fwd_body, grid=(f // TILE,), name='fwd',
        in_specs=[pl.BlockSpec((None, b, d), lambda j: (hk, 0, 0)), pl.BlockSpec((None, d, TILE), lambda j: (k1, 0, j)),
                  pl.BlockSpec((None, TILE, d), lambda j: (k2, j, 0))],
        out_specs=pl.BlockSpec((b, d), lambda j: (0, 0)), out_shape=jax.ShapeDtypeStruct((b, d), BF16),
        scratch_shapes=[pltpu.VMEM((b, d), BF16), pltpu.VMEM((b, d), F32)], compiler_params=params(),
        cost_estimate=cost(4 * b * d * f, 8 * d * f + 4 * b * d, b * f))(h, w1, w2)


def chain_body(n_fwd, nt, mixing, loss_scale, *refs):
    refs = list(refs)
    h_ref, hist_ref = refs.pop(0), None
    w1f_ref = refs.pop(0)
    w2f_refs = [refs.pop(0) for _ in range(5 if mixing else 1)]
    t_ref, w1h_ref, w2h_ref = [refs.pop(0) for _ in range(3)]
    hist_ref, a_ref, e_ref, q_ref, wire_ref = [refs.pop(0) for _ in range(5)]
    if mixing:
        p_ref = refs.pop(0)
    h_scr, n_scr, acc_scr, a_scr, w_scr, elo_scr = refs
    i = pl.program_id(0)
    j = lax.rem(i, nt)
    in_fwd = i < n_fwd * nt
    in_head = (i >= n_fwd * nt) & (i < (n_fwd + 1) * nt)
    b = h_ref.shape[0]
    half = e_ref.shape[1]
    blocks = row_blocks(b)
    thin = row_blocks(b, THIN)

    @pl.when(i == 0)
    def _():
        h_scr[...] = h_ref[...]

    @pl.when((j == 0) & (i <= n_fwd * nt))
    def _():
        for r in thin:
            x = h_scr[r, :].astype(F32)
            n_scr[r, :] = (x * inv_rms_of(x)).astype(BF16)
        acc_scr[...] = jnp.zeros_like(acc_scr)

    @pl.when(in_fwd)
    def _():
        w1 = w1f_ref[...].astype(BF16)
        if mixing:
            w2 = mix_refs(w2f_refs)
            p_ref[...] = w2
        else:
            w2 = w2f_refs[0][...]
        w2 = w2.astype(BF16)
        for r in blocks:
            a = gelu_value(mm(n_scr[r, :], w1)).astype(BF16)
            acc_scr[r, :] += mm(a, w2)

    @pl.when(in_fwd & (j == nt - 1))
    def _():
        for r in thin:
            out = (h_scr[r, :].astype(F32) + acc_scr[r, :]).astype(BF16)
            h_scr[r, :] = out
            hist_ref[r, :] = out

    @pl.when(in_head)
    def _():
        w1 = w1h_ref[...].astype(BF16)
        w2 = w2h_ref[...]
        w_scr[j] = w2
        w2 = w2.astype(BF16)
        for r in blocks:
            a = gelu_value(mm(n_scr[r, :], w1)).astype(BF16)
            a_scr[j, r, :] = a
            a_ref[r, :] = a
            acc_scr[r, :half] += mm(a, w2)

    @pl.when(in_head & (j == nt - 1))
    def _():
        for r in thin:
            out = (h_scr[r, :half].astype(F32) + acc_scr[r, :half]).astype(BF16)
            e = loss_scale * (out.astype(F32) - t_ref[r, :].astype(F32))
            e_ref[r, :] = e
            elo_scr[r, :] = e.astype(BF16)

    @pl.when(i >= (n_fwd + 1) * nt)
    def _():
        q = w_scr[j] - LEARN_RATE * mm(a_scr[j], elo_scr[...], TN)
        q_ref[...] = q
        wire_ref[...] = q.astype(BF16)


def chain(n_fwd, h, hk, target, tk, w1f, k1f, w2f, k2f, w1h, k1h, w2h, k2h, half, loss_scale, even, tile):
    b, d = h.shape[1:]
    f = w1f.shape[2]
    nt = f // tile
    mixing = isinstance(w2f, tuple)
    n_steps = n_fwd * nt

    def f_layer(i):
        return jnp.minimum(i, n_steps - 1) // nt

    def f_tile(i):
        return jnp.minimum(i, n_steps - 1) % nt

    def h_tile(i):
        return jnp.clip(i - n_steps, 0, nt - 1)

    def g_tile(i):
        return jnp.maximum(i - n_steps - nt, 0)

    in_specs = [pl.BlockSpec((None, b, d), lambda i: (hk, 0, 0)),
                pl.BlockSpec((None, d, tile), lambda i: (k1f + f_layer(i), 0, f_tile(i)))]
    if mixing:
        in_specs += [pl.BlockSpec((tile, d), lambda i: (f_tile(i), 0))] * 4 + [pl.BlockSpec(memory_space=pltpu.SMEM)]
    else:
        in_specs.append(pl.BlockSpec((None, tile, d), lambda i: (k2f + f_layer(i), f_tile(i), 0)))
    in_specs += [pl.BlockSpec((None, b, half), lambda i: (tk, 0, 0)), pl.BlockSpec((None, d, tile), lambda i: (k1h, 0, h_tile(i))),
                 pl.BlockSpec((None, tile, half), lambda i: (k2h, h_tile(i), 0))]
    out_specs = [pl.BlockSpec((None, b, d), lambda i: (f_layer(i), 0, 0)), pl.BlockSpec((b, tile), lambda i: (0, h_tile(i))),
                 pl.BlockSpec((b, half), lambda i: (0, 0))] + [pl.BlockSpec((tile, half), lambda i: (g_tile(i), 0))] * 2
    out_shape = [jax.ShapeDtypeStruct((n_fwd, b, d), BF16), jax.ShapeDtypeStruct((b, f), BF16), jax.ShapeDtypeStruct((b, half), F32),
                 jax.ShapeDtypeStruct((f, half), F32), jax.ShapeDtypeStruct((f, half), BF16)]
    if mixing:
        out_specs.append(pl.BlockSpec((tile, d), lambda i: (f_tile(i), 0)))
        out_shape.append(jax.ShapeDtypeStruct((f, d), F32))
    return pl.pallas_call(
        functools.partial(chain_body, n_fwd, nt, mixing, loss_scale), grid=((n_fwd + 2) * nt,), name='chain',
        in_specs=in_specs, out_specs=out_specs, out_shape=out_shape,
        scratch_shapes=[pltpu.VMEM((b, d), BF16), pltpu.VMEM((b, d), BF16), pltpu.VMEM((b, d), F32), pltpu.VMEM((nt, b, tile), BF16),
                        pltpu.VMEM((nt, tile, half), F32), pltpu.VMEM((b, half), BF16)],
        compiler_params=params(),
        cost_estimate=cost(2 * b * f * (2 * n_fwd * d + d + 2 * half), 8 * n_fwd * d * f + 4 * d * f + 2 * b * f + 10 * f * half, (n_fwd + 1) * b * f))(
            h, w1f, *((*w2f, even) if mixing else (w2f,)), target, w1h, w2h)


def tail_body(nt, mixing, loss_scale, *refs):
    refs = list(refs)
    a_ref, h_ref, hc_ref, t_ref, e0_ref, w1_ref, w20_ref = [refs.pop(0) for _ in range(7)]
    w21_refs = [refs.pop(0) for _ in range(5 if mixing else 1)]
    e1_ref, dz_ref, q_ref, wire_ref = [refs.pop(0) for _ in range(4)]
    if mixing:
        p_ref = refs.pop(0)
    n_scr, acc_scr, w2_scr, elo_scr = refs
    i = pl.program_id(0)
    j = lax.rem(i, nt)
    blocks = row_blocks(h_ref.shape[0])
    thin = row_blocks(h_ref.shape[0], THIN)
    half = e0_ref.shape[1]

    @pl.when(i == 0)
    def _():
        acc_scr[...] = jnp.zeros_like(acc_scr)
        for r in thin:
            x = h_ref[r, :].astype(F32)
            n_scr[r, :] = (x * inv_rms_of(x)).astype(BF16)

    @pl.when(i < nt)
    def _():
        if mixing:
            w2 = mix_refs(w21_refs)
            p_ref[...] = w2
        else:
            w2 = w21_refs[0][...]
        w2 = w2.astype(BF16)
        w2_scr[j, :, :half] = w20_ref[...].astype(BF16)
        w2_scr[j, :, half:] = w2
        acc_scr[...] += mm(a_ref[...], w2)

    @pl.when(i == nt - 1)
    def _():
        for r in thin:
            out = (hc_ref[r, :].astype(F32) + acc_scr[r, :]).astype(BF16)
            e = loss_scale * (out.astype(F32) - t_ref[r, :].astype(F32))
            e1_ref[r, :] = e
            elo_scr[r, :half] = e0_ref[r, :].astype(BF16)
            elo_scr[r, half:] = e.astype(BF16)

    @pl.when(i >= nt)
    def _():
        w1 = w1_ref[...]
        w1_lo = w1.astype(BF16)
        for r in blocks:
            _, slope = gelu_both(mm(n_scr[r, :], w1_lo))
            dz_ref[r, :] = (mm(elo_scr[r, :], w2_scr[j], NT) * slope).astype(BF16)
        q = w1 - LEARN_RATE * mm(n_scr[...], dz_ref[...], TN)
        q_ref[...] = q
        wire_ref[...] = q.astype(BF16)


def tail(act, h, hk, target, tk, e0, w1, k1, w20, k20, w21, k21, c21, half, loss_scale, even):
    b, d = h.shape[1:]
    f = w1.shape[2]
    nt = f // TILE
    mixing = isinstance(w21, tuple)

    def p_tile(i):
        return jnp.minimum(i, nt - 1)

    def g_tile(i):
        return jnp.maximum(i - nt, 0)

    in_specs = [pl.BlockSpec((b, TILE), lambda i: (0, p_tile(i))), pl.BlockSpec((None, b, d), lambda i: (hk, 0, 0)),
                pl.BlockSpec((None, b, half), lambda i: (hk, 0, 1)), pl.BlockSpec((None, b, half), lambda i: (tk, 0, 1)),
                pl.BlockSpec((b, half), lambda i: (0, 0)), pl.BlockSpec((None, d, TILE), lambda i: (k1, 0, g_tile(i))),
                pl.BlockSpec((None, TILE, half), lambda i: (k20, p_tile(i), 0))]
    if mixing:
        in_specs += [pl.BlockSpec((TILE, half), lambda i: (p_tile(i), 0))] * 4 + [pl.BlockSpec(memory_space=pltpu.SMEM)]
    else:
        in_specs.append(pl.BlockSpec((None, TILE, half), lambda i: (k21, p_tile(i), c21)))
    out_specs = [pl.BlockSpec((b, half), lambda i: (0, 0)), pl.BlockSpec((b, TILE), lambda i: (0, g_tile(i)))]
    out_specs += [pl.BlockSpec((d, TILE), lambda i: (0, g_tile(i)))] * 2
    out_shape = [jax.ShapeDtypeStruct((b, half), F32), jax.ShapeDtypeStruct((b, f), BF16), jax.ShapeDtypeStruct((d, f), F32),
                 jax.ShapeDtypeStruct((d, f), BF16)]
    if mixing:
        out_specs.append(pl.BlockSpec((TILE, half), lambda i: (p_tile(i), 0)))
        out_shape.append(jax.ShapeDtypeStruct((f, half), F32))
    return pl.pallas_call(
        functools.partial(tail_body, nt, mixing, loss_scale), grid=(2 * nt,), name='tail', in_specs=in_specs, out_specs=out_specs,
        out_shape=out_shape,
        scratch_shapes=[pltpu.VMEM((b, d), BF16), pltpu.VMEM((b, half), F32), pltpu.VMEM((nt, TILE, d), BF16), pltpu.VMEM((b, d), BF16)],
        compiler_params=params(),
        cost_estimate=cost(2 * b * f * (3 * d + half), 10 * d * f + 8 * f * half + 4 * b * f, b * f))(
            act, h, h, target, e0, w1, w20, *((*w21, even) if mixing else (w21,)))


def last_body(a_ref, dz_ref, h_ref, e0_ref, e1_ref, w1_ref, w2_ref, q_ref, wire_ref, en_ref, m_scr, elo_scr):
    j = pl.program_id(0)
    thin = row_blocks(h_ref.shape[0], THIN)
    half = e0_ref.shape[1]

    @pl.when(j == 0)
    def _():
        m_scr[...] = jnp.zeros_like(m_scr)
        elo_scr[...] = e1_ref[...].astype(BF16)

    m_scr[...] += mm(dz_ref[...], w1_ref[...].astype(BF16), NT)
    q = w2_ref[...] - LEARN_RATE * mm(a_ref[...], elo_scr[...], TN)
    q_ref[...] = q
    wire_ref[...] = q.astype(BF16)

    @pl.when(j == pl.num_programs(0) - 1)
    def _():
        for r in thin:
            step = norm_back(h_ref[r, :].astype(F32), m_scr[r, :])
            en_ref[r, :half] = e0_ref[r, :] + step[:, :half]
            en_ref[r, half:] = e1_ref[r, :] + step[:, half:]


def bwd_last(act, dz, h, hk, e0, e1, w1, k1, w2, k2, c2, half):
    b, d = h.shape[1:]
    f = w1.shape[2]
    return pl.pallas_call(
        last_body, grid=(f // TILE,), name='bwd_last',
        in_specs=[pl.BlockSpec((b, TILE), lambda j: (0, j))] * 2 + [pl.BlockSpec((None, b, d), lambda j: (hk, 0, 0))]
        + [pl.BlockSpec((b, half), lambda j: (0, 0))] * 2
        + [pl.BlockSpec((None, d, TILE), lambda j: (k1, 0, j)), pl.BlockSpec((None, TILE, half), lambda j: (k2, j, c2))],
        out_specs=[pl.BlockSpec((TILE, half), lambda j: (j, 0))] * 2 + [pl.BlockSpec((b, d), lambda j: (0, 0))],
        out_shape=[jax.ShapeDtypeStruct((f, half), F32), jax.ShapeDtypeStruct((f, half), BF16), jax.ShapeDtypeStruct((b, d), F32)],
        scratch_shapes=[pltpu.VMEM((b, d), F32), pltpu.VMEM((b, half), BF16)], compiler_params=params(),
        cost_estimate=cost(2 * b * f * (d + half), 4 * d * f + 10 * f * half + 4 * b * f))(act, dz, h, e0, e1, w1, w2)


def bwd_body(with_next, e_ref, h_ref, w1_ref, w2_ref, q1_ref, wire1_ref, q2_ref, wire2_ref, *rest):
    if with_next:
        en_ref, elo_scr, n_scr, a_scr, dz_scr, m_scr = rest
    else:
        elo_scr, n_scr, a_scr, dz_scr = rest
    j = pl.program_id(0)
    blocks = row_blocks(h_ref.shape[0])
    thin = row_blocks(h_ref.shape[0], THIN)

    @pl.when(j == 0)
    def _():
        for r in thin:
            elo_scr[r, :] = e_ref[r, :].astype(BF16)
            x = h_ref[r, :].astype(F32)
            n_scr[r, :] = (x * inv_rms_of(x)).astype(BF16)
        if with_next:
            m_scr[...] = jnp.zeros_like(m_scr)

    w1 = w1_ref[...].astype(BF16)
    w2 = w2_ref[...].astype(BF16)
    for r in blocks:
        value, slope = gelu_both(mm(n_scr[r, :], w1))
        a_scr[r, :] = value.astype(BF16)
        dz = (mm(elo_scr[r, :], w2, NT) * slope).astype(BF16)
        dz_scr[r, :] = dz
        if with_next:
            m_scr[r, :] += mm(dz, w1, NT)
    q1 = w1_ref[...] - LEARN_RATE * mm(n_scr[...], dz_scr[...], TN)
    q1_ref[...] = q1
    wire1_ref[...] = q1.astype(BF16)
    q2 = w2_ref[...] - LEARN_RATE * mm(a_scr[...], elo_scr[...], TN)
    q2_ref[...] = q2
    wire2_ref[...] = q2.astype(BF16)

    if with_next:
        @pl.when(j == pl.num_programs(0) - 1)
        def _():
            for r in thin:
                en_ref[r, :] = e_ref[r, :] + norm_back(h_ref[r, :].astype(F32), m_scr[r, :])


def bwd_layer(e, h, hk, w1, k1, w2, k2, with_next):
    b, d = h.shape[1:]
    f = w1.shape[2]
    out_specs = [pl.BlockSpec((d, TILE), lambda j: (0, j))] * 2 + [pl.BlockSpec((TILE, d), lambda j: (j, 0))] * 2
    out_shape = [jax.ShapeDtypeStruct((d, f), F32), jax.ShapeDtypeStruct((d, f), BF16),
                 jax.ShapeDtypeStruct((f, d), F32), jax.ShapeDtypeStruct((f, d), BF16)]
    scratch = [pltpu.VMEM((b, d), BF16), pltpu.VMEM((b, d), BF16), pltpu.VMEM((b, TILE), BF16), pltpu.VMEM((b, TILE), BF16)]
    if with_next:
        out_specs.append(pl.BlockSpec((b, d), lambda j: (0, 0)))
        out_shape.append(jax.ShapeDtypeStruct((b, d), F32))
        scratch.append(pltpu.VMEM((b, d), F32))
    n_mm = 5 if with_next else 4
    return pl.pallas_call(
        functools.partial(bwd_body, with_next), grid=(f // TILE,), name='bwd_mid' if with_next else 'bwd_first',
        in_specs=[pl.BlockSpec((b, d), lambda j: (0, 0)), pl.BlockSpec((None, b, d), lambda j: (hk, 0, 0)),
                  pl.BlockSpec((None, d, TILE), lambda j: (k1, 0, j)), pl.BlockSpec((None, TILE, d), lambda j: (k2, j, 0))],
        out_specs=out_specs, out_shape=out_shape, scratch_shapes=scratch, compiler_params=params(),
        cost_estimate=cost(2 * n_mm * b * d * f, 20 * d * f, b * f))(e, h, w1, w2)


def mix_vals(own, lead, trail, near, even, direct):
    row, far = jnp.where(direct, lead, trail), jnp.where(direct, trail, lead)
    first, second = jnp.where(even, far, near), jnp.where(even, near, far)
    row = row.astype(F32)
    return (own + first.astype(F32) + second.astype(F32) + row + row) / 5.0


def mix_refs(refs):
    return mix_vals(*[r[...] for r in refs[:4]], refs[4][0] == 1, refs[4][1] == 1)


def place_body(own_ref, lead_ref, trail_ref, near_ref, sel_ref, *rest):
    rest[-1][...] = mix_refs([own_ref, lead_ref, trail_ref, near_ref, sel_ref])


def place(stack, shape, layer, col, own, recv, even):
    r, c = own.shape
    tr = r // 4
    spec = pl.BlockSpec((tr, c), lambda i: (i, 0))
    args = [own, *recv, even]
    in_specs = [spec] * 4 + [pl.BlockSpec(memory_space=pltpu.SMEM)]
    aliases = {}
    if stack is not None:
        args.append(stack)
        in_specs.append(pl.BlockSpec(memory_space=pl.ANY))
        aliases = {5: 0}
    return pl.pallas_call(
        place_body, grid=(4,), in_specs=in_specs,
        out_specs=pl.BlockSpec((None, tr, c), lambda i: (layer, i, col)), out_shape=jax.ShapeDtypeStruct(shape, F32),
        input_output_aliases=aliases, compiler_params=params(), name='place',
        cost_estimate=cost(5 * r * c, 14 * r * c))(*args)


def solution(mesh):
    n_rows = mesh.shape['row']
    n_cols = mesh.shape['col']
    near_pairs = [(i, i + 1 - 2 * (i % 2)) for i in range(n_cols)]
    far_pairs = [(i, (i - 1 + 2 * (i % 2)) % n_cols) for i in range(n_cols)]
    lead_pairs, trail_pairs = [], []
    for r in range(n_rows):
        for c, far in far_pairs:
            here, across, other = r * n_cols + c, (r + 1) % n_rows * n_cols + c, r * n_cols + far
            lead_pairs.append((here, across if c % 4 in (1, 2) else other))
            trail_pairs.append((here, other if c % 4 in (1, 2) else across))

    def lo_copy(weight):
        return weight[0].astype(BF16)

    def after(value, *others):
        return lax.optimization_barrier((value,) + others)[0]

    def send(wire):
        lead = lax.ppermute(wire, ('row', 'col'), lead_pairs)
        trail = lax.ppermute(wire, ('row', 'col'), trail_pairs)
        near = lax.ppermute(wire, 'col', near_pairs)
        return lead, trail, near

    def device_fn(w_one, w_two, inputs, targets):
        n_layers, d, _ = w_one.shape[2:]
        last = n_layers - 1
        half = d // 2
        n_steps, b = inputs.shape[2:4]
        loss_scale = 2.0 / (b * d)
        stack_one, stack_two = w_one[0, 0], w_two[0, 0]
        x_all, t_all = inputs[0, 0], targets[0, 0]
        col = lax.axis_index('col')
        even = jnp.stack([1 - col % 2, (col + 1) // 2 % 2]).astype(jnp.int32)
        one = [(stack_one, k) for k in range(n_layers)]
        two = [(stack_two, k) for k in range(last)]
        halves = [(stack_two, last), (stack_two, last, 1)]
        for step in range(n_steps):
            recvs, names, own, outs = [], [], {}, {}
            final = step == n_steps - 1

            def settle(k):
                name = names[k]
                if name[0] == 'one':
                    outs['one'] = place(outs.get('one'), stack_one.shape, name[1], 0, own[name], recvs[k], even)
                else:
                    layer, col = (last, int(name[1])) if name[0] == 'h' else (name[1], 0)
                    outs['two'] = place(outs.get('two'), stack_two.shape, layer, col, own[name], recvs[k], even)

            def push(name, q, wire, gate=None):
                if gate is not None and final:
                    settle(gate)
                    kinds = sorted(outs)
                    wire, *vals = lax.optimization_barrier((wire, *recvs[gate], *[outs[k] for k in kinds]))
                    outs.update(zip(kinds, vals[3:]))
                elif gate is not None:
                    wire = after(wire, *recvs[gate])
                recvs.append(send(wire))
                names.append(name)
                own[name] = q

            hidden = [(x_all, step)]
            if step == 0:
                hist, act, e0, q, wire = chain(last, *hidden[0], t_all, step, stack_one, 0, stack_two, 0, stack_one, last, stack_two, last, half, loss_scale, even, 2 * TILE)
                hidden += [(hist, l) for l in range(last)]
            else:
                for l in range(last - 1):
                    hidden.append((fwd_layer(*hidden[l], *one[l], *two[l])[None], 0))
                hist, act, e0, q, wire, mixed_two = chain(1, *hidden[last - 1], t_all, step, lo_copy(one[last - 1]), 0, two[last - 1], 0, lo_copy(one[last]), 0, *halves[0], half, loss_scale, even, TILE)
                two[last - 1] = (mixed_two[None], 0)
                hidden.append((hist, 0))
            push('h0', q, wire)
            res = tail(act, *hidden[last], t_all, step, e0, *one[last], *halves[0], *halves[1], half, loss_scale, even)
            e1, dz = res[:2]
            push(('one', last), *res[2:4])
            if step > 0:
                halves[1] = (res[4][None], 0, 0)
            ready = {}
            q, wire, err = bwd_last(act, dz, *hidden[last], e0, e1, *one[last], *halves[1], half)
            ready['h1'] = (q, wire)
            for l in reversed(range(last)):
                res = bwd_layer(err, *hidden[l], *one[l], *two[l], l > 0)
                ready['one', l], ready['two', l] = res[0:2], res[2:4]
                if l > 0:
                    err = res[4]
            early = ('one', last - 1)
            order = [early] + [(kind, l) for l in range(last) for kind in ('one', 'two') if (kind, l) != early] + ['h1']
            for name in order:
                push(name, *ready[name], gate=len(recvs) - 2)
            if not final:
                parts = {name: (own[name], *recv) for name, recv in zip(names, recvs)}
                deferred = ('h1', ('two', last - 1))
                mixed = {name: mix_vals(*vals, even[0] == 1, even[1] == 1)[None] for name, vals in parts.items() if name not in deferred}
                one = [(mixed['one', l], 0) for l in range(n_layers)]
                two = [(mixed['two', l], 0) for l in range(last - 1)] + [parts['two', last - 1]]
                halves = [(mixed['h0'], 0), (parts['h1'], 0, 0)]
        for k in range(len(names) - 2, len(names)):
            settle(k)
        return outs['one'][None, None], outs['two'][None, None]

    grid_spec = P('row', 'col')
    return jax.shard_map(device_fn, mesh=mesh, in_specs=(grid_spec, grid_spec, grid_spec, grid_spec), out_specs=(grid_spec, grid_spec), check_vma=False)
```
